32 devices in a mesh: dp: 16 (over z, y, x), shard: 2 (over core).
Axes of the slice: x: 2, y: 2, z: 4, core: 2. Of those that a mesh axis runs over, the one named last changes fastest.
Arguments:
- features: bfloat16 [65536, 1024], P('dp'), may hold values from -150 to 150
- shared_weight: bfloat16 [1024, 2048], P(None, 'shard'), may hold values from -0.1875 to 0.1875
- task_heads: bfloat16 [6, 2048], P(None, 'shard'), may hold values from -0.4 to 0.4
- labels: int32 [65536, 6], P('dp'), may hold values from 0 to 1
- task_masks: int32 [65536, 6], P('dp'), may hold values from 0 to 1
- task_weights: float32 [6], replicated, may hold values from 0.5 to 2
- initial_losses: float32 [6], replicated, may hold values from 0.2 to 1
Outputs:
- update: float32 [1024, 2048], P('dp', 'shard')
- new_weights: float32 [6], replicated
The draws below stay inside these ranges and needn't reach their ends.
All inputs are finite; a program needn't handle non-finite values.
Results may differ from the reference program's by a relative error of at most 0.00089.
Values sent between devices are 32-bit elements; how exact they have to be, the bound alone decides.
A program may use at most 256 MiB of HBM per device.

```python
import math
import jax
import jax.numpy as jnp
from jax import lax

DIN = 1024
DH = 2048
TASKS = 6
SAMPLES_DEV = 4096
SAMPLES = 65536
N_DP = 16


def draw_features(key, part):
    subkeys = jax.random.split(key, 3)
    total_rows = SAMPLES_DEV * N_DP
    row_ids = jnp.arange(total_rows)
    column_ids = jnp.arange(DIN)
    roughness = jax.random.uniform(subkeys[1], (DIN,), jnp.float32, -0.5, 0.5)
    column_scale = jnp.exp(math.log(3.0) * column_ids.astype(jnp.float32) / (DIN - 1) + math.log(4.0) * roughness)
    pairing = jax.random.permutation(subkeys[2], N_DP)
    spike_gain = jnp.where(pairing[row_ids // SAMPLES_DEV][:, None] == (column_ids // (DIN // N_DP))[None, :], 3.0, 1.0)
    base_draw = jax.random.truncated_normal(subkeys[0], -4.0, 4.0, (total_rows, DIN), jnp.float32)
    return (base_draw * column_scale[None, :] * spike_gain).astype(jnp.bfloat16)


def draw_task_heads(key, part):
    subkeys = jax.random.split(key, 2)
    column_ids = jnp.arange(DH).astype(jnp.float32)
    roughness = jax.random.uniform(subkeys[1], (DH,), jnp.float32, -0.5, 0.5)
    column_scale = jnp.exp(math.log(3.0) * column_ids / (DH - 1) + math.log(2.0) * roughness)
    base_draw = jax.random.truncated_normal(subkeys[0], -4.0, 4.0, (TASKS, DH), jnp.float32)
    values = base_draw * column_scale[None, :] / math.sqrt(DH)
    return jnp.clip(values, -0.3984375, 0.3984375).astype(jnp.bfloat16)


def draw_task_masks(key, part):
    total_rows = SAMPLES_DEV * N_DP
    row_ids = jnp.arange(total_rows, dtype=jnp.int32)
    threshold = 250 + 500 * row_ids // (total_rows - 1)
    drawn = jax.random.randint(key, (total_rows, TASKS), 0, 1000, dtype=jnp.int32)
    return (drawn < threshold[:, None]).astype(jnp.int32)


def touch_ends(array, stream_key, smallest, high):
    longest = array.shape.index(max(array.shape))
    spots = []
    for shift in (0, 1):
        where = [jax.random.randint(jax.random.fold_in(stream_key, axis), (), 0, length) for axis, length in enumerate(array.shape)]
        where[longest] = (where[longest] + shift) % array.shape[longest]
        spots.append(tuple(where))
    return array.at[spots[0]].set(smallest).at[spots[1]].set(high)


def shard_levels(key, shape, shards, low, top_value):
    gain, own = 1.0, jax.random.fold_in(key, 6)
    for dim, parts in shards:
        steps = jnp.exp(jax.random.uniform(jax.random.fold_in(own, dim), (parts,), jnp.float32, low / len(shards), top_value / len(shards)))
        gain = gain * jnp.repeat(steps, shape[dim] // parts).reshape([-1 if axis == dim else 1 for axis in range(len(shape))])
    return gain


def gaussian(stream_key, extent, deviation, most, shards=(), held_as=jnp.bfloat16):
    loudness = shard_levels(stream_key, extent, shards, -0.22, 0.18) if shards else 1.0
    values = jax.random.normal(stream_key, extent, jnp.float32) * deviation * loudness
    return jnp.minimum(jnp.maximum(values, -most), most).astype(held_as)


def setup_inputs(seed: int = 0) -> dict:
    splits = jax.random.split(jax.random.key(seed), 8)
    features = draw_features(jax.random.fold_in(splits[7], 71), 0)
    shared_weight = gaussian(splits[1], (DIN, DH), DIN ** -0.5, 0.1875, ((1, 2),))
    task_heads = draw_task_heads(jax.random.fold_in(splits[7], 71), 0)
    labels = touch_ends(jax.random.randint(splits[3], (SAMPLES, TASKS), 0, 2), jax.random.fold_in(splits[3], 1), 0, 1).astype(jnp.int32)
    task_masks = draw_task_masks(jax.random.fold_in(splits[7], 71), 0)
    task_weights = jnp.clip(jnp.exp(jax.random.uniform(splits[5], (TASKS,), jnp.float32, math.log(0.5), math.log(2.0))), 0.5, 2.0)
    initial_losses = jnp.clip(jnp.exp(jax.random.uniform(splits[6], (TASKS,), jnp.float32, math.log(0.2), math.log(1.0))), 0.2, 1.0)
    return dict(features=features, shared_weight=shared_weight, task_heads=task_heads, labels=labels, task_masks=task_masks, task_weights=task_weights, initial_losses=initial_losses)


epsilon = 1e-06
learn_rate = 0.5
asymmetry = 1.5

def silu_parts(preact):
    sigmoid_pre = jax.nn.sigmoid(preact)
    return (preact * sigmoid_pre, sigmoid_pre * (1.0 + preact * (1.0 - sigmoid_pre)))

def renew_weights(losses, squares, task_weights, initial_losses, entries):
    root_mean = jnp.sqrt(squares / entries + epsilon)
    scaled = task_weights * root_mean
    average = jnp.mean(scaled)
    loss_ratio = losses / initial_losses
    relative = loss_ratio / jnp.mean(loss_ratio)
    target = average * relative ** asymmetry
    distance = (scaled - target) / average
    raised = task_weights * jnp.exp(-learn_rate * distance)
    return raised.shape[0] * raised / jnp.sum(raised)

def reference(features, shared_weight, task_heads, labels, task_masks, task_weights, initial_losses):
    blocks = features.reshape(N_DP, SAMPLES_DEV, DIN)
    label_blocks = labels.reshape(N_DP, SAMPLES_DEV, TASKS)
    mask_blocks = task_masks.reshape(N_DP, SAMPLES_DEV, TASKS)
    heads_wide = task_heads.astype(jnp.float32)

    def block_step(running, inputs):
        grad_sum, loss_sum = running
        rows_in, label_rows, mask_rows = inputs
        preact = jnp.dot(rows_in, shared_weight, preferred_element_type=jnp.float32)
        activated, silu_slope = silu_parts(preact)
        hidden = activated.astype(jnp.bfloat16)
        logits = jnp.dot(hidden, task_heads.T, preferred_element_type=jnp.float32)
        targets = label_rows.astype(jnp.float32)
        mask_float = mask_rows.astype(jnp.float32)
        loss_sum = loss_sum + lax.optimization_barrier(jnp.sum(mask_float * (jax.nn.softplus(logits) - targets * logits), axis=0))
        errors = mask_float * (jax.nn.sigmoid(logits) - targets)
        back_terms = (errors[:, :, None] * silu_slope[:, None, :] * heads_wide[None]).astype(jnp.bfloat16)
        back_flat = back_terms.reshape(SAMPLES_DEV, TASKS * DH)
        grad_sum = grad_sum + lax.dot_general(rows_in, back_flat, (((0,), (0,)), ((), ())), preferred_element_type=jnp.float32)
        return ((grad_sum, loss_sum), None)
    start_state = (jnp.zeros((DIN, TASKS * DH), jnp.float32), jnp.zeros((TASKS,), jnp.float32))
    (grad_sum, loss_sum), unused = lax.scan(block_step, start_state, (blocks, label_blocks, mask_blocks))
    gradients = grad_sum.reshape(DIN, TASKS, DH)
    losses = loss_sum / SAMPLES
    squares = lax.optimization_barrier(jnp.sum(gradients * gradients, axis=(0, 2)))
    new_weights = renew_weights(losses, squares, task_weights, initial_losses, DIN * DH)
    combined = jnp.einsum('t,rtc->rc', new_weights, gradients, precision=lax.Precision.HIGHEST)
    update = combined * lax.rsqrt(jnp.mean(combined * combined) + epsilon)
    return (update, new_weights)
```

```python
import functools
import jax
import jax.numpy as jnp
from jax import lax
from jax.experimental import pallas as pl
from jax.experimental.pallas import tpu as pltpu
from jax.sharding import PartitionSpec as P

epsilon = 1e-06
learn_rate = 0.5
asymmetry = 1.5
MESH = pl.DeviceIdType.MESH
LAGS = (3, 6, 8, 10)


def silu_parts(preact):
    sigmoid_pre = jax.nn.sigmoid(preact)
    return (preact * sigmoid_pre, sigmoid_pre * (1.0 + preact * (1.0 - sigmoid_pre)))


def exchange_orders(task_count, levels):
    if levels == 4:
        table = ((0, 1, 2, 3), (1, 0, 2, 3), (2, 0, 1, 3), (0, 1, 2, 3), (1, 0, 2, 3), (2, 1, 0, 3))
        return [table[task % 6] for task in range(task_count)]
    return [tuple((task + level) % levels for level in range(levels)) for task in range(task_count)]


def stage_lags(levels):
    if levels == 4:
        return LAGS
    return tuple(3 + 2 * level for level in range(levels))


def partner_of(me, bit):
    mine = (me // (1 << bit)) % 2
    return me + (1 - 2 * mine) * (1 << bit)


def reduce_kernel(
    task_count,
    levels,
    shard_levels,
    entries,
    features,
    slope,
    errors,
    heads,
    stats,
    weights,
    initial,
    update,
    renewed,
    turned,
    rows_in,
    slope_in,
    terms,
    grads,
    *rest,
):
    landed = rest[:levels]
    mine_sum, their_sum, row_sem, slope_sem, send_sem, recv_sem, sum_send, sum_recv = rest[levels:]
    me = lax.axis_index("dp")
    my_shard = lax.axis_index("shard")
    samples, width_in = features.shape
    columns = terms.shape[1]
    blocks = slope.shape[1] // columns
    row_block = rows_in.shape[1]
    tile = min(256, width_in)
    tiles = width_in // tile
    tile_bits = tiles.bit_length() - 1
    orders = exchange_orders(task_count, levels)
    lags = stage_lags(levels)
    dp_partner = [partner_of(me, bit) for bit in range(levels)]
    shard_partner = [partner_of(my_shard, bit) for bit in range(shard_levels)]
    my_bit = [(me // (1 << bit)) % 2 for bit in range(levels)]

    barrier = pltpu.get_barrier_semaphore()
    for bit in range(levels):
        pl.semaphore_signal(
            barrier, inc=1, device_id=(dp_partner[bit], my_shard), device_id_type=MESH
        )
    for bit in range(shard_levels):
        pl.semaphore_signal(
            barrier, inc=1, device_id=(me, shard_partner[bit]), device_id_type=MESH
        )

    def load_rows(index):
        return pltpu.make_async_copy(
            features.at[pl.ds(index * row_block, row_block), :],
            rows_in.at[index % 2],
            row_sem.at[index % 2],
        )

    def load_slope(block, slot):
        return pltpu.make_async_copy(
            slope.at[:, pl.ds(pl.multiple_of(block * columns, columns), columns)],
            slope_in.at[slot],
            slope_sem.at[slot],
        )

    load_rows(0).start()
    for index in range(samples // row_block):
        if index + 1 < samples // row_block:
            load_rows(index + 1).start()
        load_rows(index).wait()
        turned[:, index * row_block : (index + 1) * row_block] = rows_in[index % 2].T
        if index == 0:
            load_slope(0, 0).start()
    pl.semaphore_wait(barrier, levels + shard_levels)

    def compute(block, slot, task):
        head = heads[task : task + 1, pl.ds(pl.multiple_of(block * columns, columns), columns)]

        def fill(step, carry):
            rows = pl.ds(pl.multiple_of(step * 256, 256), 256)
            scaled = errors[rows, task : task + 1] * slope_in[slot, rows, :]
            terms[rows, :] = (scaled * head).astype(jnp.bfloat16)
            return carry

        lax.fori_loop(0, samples // 256, fill, 0)

        def multiply(step, carry):
            rows = pl.ds(pl.multiple_of(step * tile, tile), tile)
            product = jnp.dot(turned[rows, :], terms[...], preferred_element_type=jnp.float32)
            high = tuple((step // (1 << bit)) % 2 for bit in range(tile_bits - 1, -1, -1))
            shape = grads.shape[1 + tile_bits :]
            grads[(task,) + high] = product.reshape(shape)
            return carry

        lax.fori_loop(0, tiles, multiply, 0)

    def part_of(block, task, stage, side):
        order = orders[task]
        left = [bit for bit in range(levels - 1, -1, -1) if bit not in order[:stage]]
        chosen = [side if bit == order[stage] else slice(None) for bit in left]
        if stage == 0:
            return grads, (task, *chosen)
        return landed[stage - 1], (block * task_count + task, *chosen)

    def exchange(block, task, stage):
        bit = orders[task][stage]
        chunk = block * task_count + task
        source, where = part_of(block, task, stage, 1 - my_bit[bit])
        return pltpu.make_async_remote_copy(
            src_ref=source.at[where],
            dst_ref=landed[stage].at[chunk],
            send_sem=send_sem.at[chunk, stage],
            recv_sem=recv_sem.at[chunk, stage],
            device_id=(dp_partner[bit], my_shard),
            device_id_type=MESH,
        )

    def combine(block, task, stage):
        bit = orders[task][stage]
        chunk = block * task_count + task
        exchange(block, task, stage).wait()
        source, where = part_of(block, task, stage, my_bit[bit])
        landed[stage][chunk] = landed[stage][chunk] + source[where]
        if stage + 1 < levels:
            exchange(block, task, stage + 1).start()

    def stages(block, task, guard):
        for stage in range(levels):
            earlier = task - lags[stage]
            of_task = earlier % task_count
            of_block = block + earlier // task_count
            if guard:

                @pl.when(of_block >= 0)
                def _():
                    combine(of_block, of_task, stage)
            else:
                if of_block < blocks and of_block >= 0:
                    combine(of_block, of_task, stage)

    def block_step(block, carry):
        slot = block % 2
        load_slope(block, slot).wait()

        @pl.when(block + 1 < blocks)
        def _():
            load_slope(block + 1, 1 - slot).start()

        for task in range(task_count):
            compute(block, slot, task)
            exchange(block, task, 0).start()
            stages(block, task, True)
        return carry

    lax.fori_loop(0, blocks, block_step, 0)
    for tick in range(lags[-1]):
        stages(blocks + tick // task_count, tick % task_count, False)

    final = landed[levels - 1]
    row = lax.broadcasted_iota(jnp.int32, (8, 128), 0)
    lane = lax.broadcasted_iota(jnp.int32, (8, 128), 1)
    total = stats[...]
    for one in range(task_count):
        for other in range(one, task_count):
            product = final[one] * final[other]
            for block in range(1, blocks):
                base = block * task_count
                product = product + final[base + one] * final[base + other]
            inner = jnp.sum(jnp.sum(product, axis=0, keepdims=True), axis=1, keepdims=True)
            here = ((row == one) & (lane == other)) | ((row == other) & (lane == one))
            total = jnp.where(here, inner, total)
    mine_sum[0] = total
    steps = [(me, partner) for partner in shard_partner]
    steps += [(partner, my_shard) for partner in dp_partner]
    for step, device in enumerate(steps):
        copy = pltpu.make_async_remote_copy(
            src_ref=mine_sum.at[step],
            dst_ref=their_sum.at[step],
            send_sem=sum_send.at[step],
            recv_sem=sum_recv.at[step],
            device_id=device,
            device_id_type=MESH,
        )
        copy.start()
        copy.wait()
        total = total + their_sum[step]
        if step + 1 < len(steps):
            mine_sum[step + 1] = total

    is_task = row[:, :1] < task_count
    diagonal = jnp.sum(jnp.where(row == lane, total, 0.0), axis=1, keepdims=True)
    losses = total[:, task_count : task_count + 1]

    def over_tasks(values):
        return jnp.sum(jnp.where(is_task, values, 0.0), axis=0, keepdims=True)

    root_mean = jnp.sqrt(diagonal / entries + epsilon)
    scaled = weights[...] * root_mean
    average = over_tasks(scaled) / task_count
    loss_ratio = losses / initial[...]
    relative = loss_ratio / (over_tasks(loss_ratio) / task_count)
    target = average * (relative * jnp.sqrt(relative))
    distance = (scaled - target) / average
    raised = weights[...] * jnp.exp(-learn_rate * distance)
    fresh = task_count * raised / over_tasks(raised)
    renewed[...] = jnp.broadcast_to(fresh, (8, 128))
    fresh = jnp.where(is_task, fresh, 0.0)
    across = jnp.sum(jnp.where(row == lane, fresh, 0.0), axis=0, keepdims=True)
    gram = jnp.where((row < task_count) & (lane < task_count), total, 0.0)
    inner = jnp.sum(gram * across, axis=1, keepdims=True)
    mean_square = jnp.sum(inner * fresh, axis=0, keepdims=True) / entries
    gain = lax.rsqrt(mean_square + epsilon)
    for block in range(blocks):
        base = block * task_count
        combined = fresh[0:1] * final[base]
        for task in range(1, task_count):
            combined = combined + fresh[task : task + 1] * final[base + task]
        update[:, block * columns : (block + 1) * columns] = combined * gain


def reduce_gradients(
    features, slope, errors, heads, stats, weights, initial, levels, shard_levels, entries
):
    samples, width_in = features.shape
    local_hidden = slope.shape[1]
    task_count = heads.shape[0]
    columns = min(256, local_hidden)
    chunks = (local_hidden // columns) * task_count
    rows = width_in >> levels
    row_block = min(512, samples)
    sums = levels + shard_levels
    vmem = pl.BlockSpec(memory_space=pltpu.VMEM)
    anywhere = pl.BlockSpec(memory_space=pl.ANY)
    landed = [
        pltpu.VMEM((chunks,) + (2,) * (levels - 1 - stage) + (rows, columns), jnp.float32)
        for stage in range(levels)
    ]
    return pl.pallas_call(
        functools.partial(reduce_kernel, task_count, levels, shard_levels, entries),
        out_shape=(
            jax.ShapeDtypeStruct((rows, local_hidden), jnp.float32),
            jax.ShapeDtypeStruct((8, 128), jnp.float32),
        ),
        in_specs=[anywhere, anywhere, vmem, vmem, vmem, vmem, vmem],
        out_specs=(vmem, vmem),
        scratch_shapes=[
            pltpu.VMEM((width_in, samples), jnp.bfloat16),
            pltpu.VMEM((2, row_block, width_in), jnp.bfloat16),
            pltpu.VMEM((2, samples, columns), jnp.float32),
            pltpu.VMEM((samples, columns), jnp.bfloat16),
            pltpu.VMEM((task_count,) + (2,) * levels + (rows, columns), jnp.float32),
            *landed,
            pltpu.VMEM((sums, 8, 128), jnp.float32),
            pltpu.VMEM((sums, 8, 128), jnp.float32),
            pltpu.SemaphoreType.DMA((2,)),
            pltpu.SemaphoreType.DMA((2,)),
            pltpu.SemaphoreType.DMA((chunks, levels)),
            pltpu.SemaphoreType.DMA((chunks, levels)),
            pltpu.SemaphoreType.DMA((sums,)),
            pltpu.SemaphoreType.DMA((sums,)),
        ],
        compiler_params=pltpu.CompilerParams(
            collective_id=0, has_side_effects=True, vmem_limit_bytes=62 * 1024 * 1024
        ),
        name="reduce_gradients",
    )(features, slope, errors, heads, stats, weights, initial)


def sum_over_shard(partial, shard_count):
    if shard_count == 2:
        return partial + lax.ppermute(partial, "shard", [(0, 1), (1, 0)])
    return lax.psum(partial, "shard")


def on_device(
    features, shared_weight, task_heads, labels, task_masks, task_weights, initial_losses
):
    shard_count = lax.axis_size("shard")
    replica_count = lax.axis_size("dp")
    width_in = features.shape[1]
    local_hidden = shared_weight.shape[1]
    task_count = task_heads.shape[0]
    entries = width_in * local_hidden * shard_count
    total_samples = features.shape[0] * replica_count
    levels = replica_count.bit_length() - 1
    shard_levels = shard_count.bit_length() - 1
    preact = jnp.dot(features, shared_weight, preferred_element_type=jnp.float32)
    activated, silu_slope = silu_parts(preact)
    hidden = activated.astype(jnp.bfloat16)
    partial_logits = lax.dot_general(
        task_heads, hidden, (((1,), (1,)), ((), ())), preferred_element_type=jnp.float32
    )
    logits = sum_over_shard(partial_logits, shard_count)
    targets = labels.T.astype(jnp.float32)
    mask_float = task_masks.T.astype(jnp.float32)
    loss_part = (
        jnp.sum(mask_float * (jax.nn.softplus(logits) - targets * logits), axis=1) / total_samples
    )
    errors = (mask_float * (jax.nn.sigmoid(logits) - targets)).T
    lane = lax.broadcasted_iota(jnp.int32, (8, 128), 1)
    padding = 8 - task_count
    loss_column = jnp.pad(loss_part / shard_count, (0, padding))[:, None]
    stats = jnp.where(lane == task_count, loss_column, 0.0)
    update, renewed = reduce_gradients(
        features,
        silu_slope,
        errors,
        task_heads.astype(jnp.float32),
        stats,
        jnp.pad(task_weights, (0, padding), constant_values=1.0)[:, None],
        jnp.pad(initial_losses, (0, padding), constant_values=1.0)[:, None],
        levels,
        shard_levels,
        entries,
    )
    return (update, renewed[:task_count, 0])


def solution(mesh):
    return jax.shard_map(
        on_device,
        mesh=mesh,
        in_specs=(
            P("dp", None),
            P(None, "shard"),
            P(None, "shard"),
            P("dp", None),
            P("dp", None),
            P(),
            P(),
        ),
        out_specs=(P("dp", "shard"), P()),
        check_vma=False,
    )
```

```python
import functools
import jax
import jax.numpy as jnp
from jax import lax
from jax.experimental import pallas as pl
from jax.experimental.pallas import tpu as pltpu
from jax.sharding import PartitionSpec as P

epsilon = 1e-06
learn_rate = 0.5
asymmetry = 1.5
MESH = pl.DeviceIdType.MESH
LAGS = (4, 8, 12, 16)
ROW_BLOCK = 512
FILL_ROWS = 1024


def silu_parts(preact):
    sigmoid_pre = jax.nn.sigmoid(preact)
    return (preact * sigmoid_pre, sigmoid_pre * (1.0 + preact * (1.0 - sigmoid_pre)))


def exchange_orders(count, levels):
    if levels == 4:
        table = ((0, 1, 2, 3), (1, 0, 2, 3), (2, 0, 1, 3), (0, 1, 2, 3), (1, 0, 2, 3), (2, 1, 0, 3))
        return [table[index % 6] for index in range(count)]
    return [tuple((index + level) % levels for level in range(levels)) for index in range(count)]


def stage_lags(levels):
    if levels == 4:
        return LAGS
    return tuple(4 + 4 * level for level in range(levels))


def partner_of(me, bit):
    mine = (me // (1 << bit)) % 2
    return me + (1 - 2 * mine) * (1 << bit)


def reduce_kernel(
    task_count,
    levels,
    shard_levels,
    entries,
    total_samples,
    features,
    shared,
    heads,
    labels,
    masks,
    weights,
    initial,
    update,
    renewed,
    turned,
    rows_in,
    slope,
    errors,
    logits,
    other_logits,
    terms,
    grads,
    *rest,
):
    landed = rest[:levels]
    pair_sum, other_sum, all_sums, row_sem, send_sem, recv_sem = rest[levels : levels + 6]
    logit_send, logit_recv, pair_send, pair_recv, share_send, share_recv = rest[levels + 6 :]
    me = lax.axis_index("dp")
    my_shard = lax.axis_index("shard")
    replicas = 1 << levels
    samples, width_in = features.shape
    local_hidden = shared.shape[1]
    columns = terms.shape[1]
    blocks = local_hidden // columns
    row_block = rows_in.shape[1]
    row_blocks = samples // row_block
    lanes = grads.shape[-1]
    halves = columns // lanes
    pieces = task_count * halves
    slots = grads.shape[0]
    tile = min(512, width_in)
    tiles = width_in // tile
    tile_bits = tiles.bit_length() - 1
    orders = exchange_orders(pieces, levels)
    lags = stage_lags(levels)
    dp_partner = [partner_of(me, bit) for bit in range(levels)]
    shard_partner = [partner_of(my_shard, bit) for bit in range(shard_levels)]
    my_bit = [(me // (1 << bit)) % 2 for bit in range(levels)]

    barrier = pltpu.get_barrier_semaphore()
    for offset in range(1, replicas):
        pl.semaphore_signal(
            barrier, inc=1, device_id=((me + offset) % replicas, my_shard), device_id_type=MESH
        )
    for bit in range(shard_levels):
        pl.semaphore_signal(
            barrier, inc=1, device_id=(me, shard_partner[bit]), device_id_type=MESH
        )

    def load_rows(index):
        return pltpu.make_async_copy(
            features.at[pl.ds(pl.multiple_of(index * row_block, row_block), row_block), :],
            rows_in.at[index % 2],
            row_sem.at[index % 2],
        )

    load_rows(0).start()

    def front(index, carry):
        @pl.when(index + 1 < row_blocks)
        def _():
            load_rows(index + 1).start()

        load_rows(index).wait()
        inputs = rows_in[index % 2]
        rows = pl.ds(pl.multiple_of(index * row_block, row_block), row_block)
        turned[:, rows] = inputs.T
        partial = jnp.zeros((row_block, task_count), jnp.float32)
        for block in range(blocks):
            part = slice(block * columns, (block + 1) * columns)
            preact = jnp.dot(inputs, shared[:, part], preferred_element_type=jnp.float32)
            activated, silu_slope = silu_parts(preact)
            slope[rows, part] = silu_slope
            partial = partial + lax.dot_general(
                activated.astype(jnp.bfloat16),
                heads[:, part],
                (((1,), (1,)), ((), ())),
                preferred_element_type=jnp.float32,
            )
        logits[0, :, rows] = partial.T
        return carry

    lax.fori_loop(0, row_blocks, front, 0)
    pl.semaphore_wait(barrier, replicas - 1 + shard_levels)
    for level in range(shard_levels):
        copy = pltpu.make_async_remote_copy(
            src_ref=logits.at[level],
            dst_ref=other_logits.at[level],
            send_sem=logit_send.at[level],
            recv_sem=logit_recv.at[level],
            device_id=(me, shard_partner[level]),
            device_id_type=MESH,
        )
        copy.start()
        copy.wait()
        logits[level + 1] = logits[level] + other_logits[level]
    whole = logits[shard_levels]
    targets = labels[...].astype(jnp.float32)
    mask_float = masks[...].astype(jnp.float32)
    loss = jnp.sum(
        mask_float * (jax.nn.softplus(whole) - targets * whole), axis=1, keepdims=True
    ) / (total_samples * (1 << shard_levels))
    flat_errors = mask_float * (jax.nn.sigmoid(whole) - targets)
    errors[...] = flat_errors.T

    fill_rows = min(FILL_ROWS, samples)

    def compute(block, task):
        part = pl.ds(pl.multiple_of(block * columns, columns), columns)
        head = heads[task : task + 1, part].astype(jnp.float32)

        def fill(step, carry):
            rows = pl.ds(pl.multiple_of(step * fill_rows, fill_rows), fill_rows)
            scaled = errors[rows, task : task + 1] * slope[rows, part]
            terms[rows, :] = (scaled * head).astype(jnp.bfloat16)
            return carry

        lax.fori_loop(0, samples // fill_rows, fill, 0)

        def multiply(step, carry):
            rows = pl.ds(pl.multiple_of(step * tile, tile), tile)
            product = jnp.dot(turned[rows, :], terms[...], preferred_element_type=jnp.float32)
            high = tuple((step // (1 << bit)) % 2 for bit in range(tile_bits - 1, -1, -1))
            shape = grads.shape[2 + tile_bits :]
            for half in range(halves):
                part = product[:, half * lanes : (half + 1) * lanes]
                grads[(task % slots, half) + high] = part.reshape(shape)
            return carry

        lax.fori_loop(0, tiles, multiply, 0)

    def part_of(block, piece, stage, side):
        order = orders[piece]
        left = [bit for bit in range(levels - 1, -1, -1) if bit not in order[:stage]]
        chosen = [side if bit == order[stage] else slice(None) for bit in left]
        if stage == 0:
            return grads, ((piece // halves) % slots, piece % halves, *chosen)
        return landed[stage - 1], (block * pieces + piece, *chosen)

    def exchange(block, piece, stage):
        bit = orders[piece][stage]
        index = block * pieces + piece
        source, where = part_of(block, piece, stage, 1 - my_bit[bit])
        return pltpu.make_async_remote_copy(
            src_ref=source.at[where],
            dst_ref=landed[stage].at[index],
            send_sem=send_sem.at[index, stage],
            recv_sem=recv_sem.at[index, stage],
            device_id=(dp_partner[bit], my_shard),
            device_id_type=MESH,
        )

    def combine(block, piece, stage):
        bit = orders[piece][stage]
        index = block * pieces + piece
        exchange(block, piece, stage).wait()
        source, where = part_of(block, piece, stage, my_bit[bit])
        landed[stage][index] = landed[stage][index] + source[where]
        if stage + 1 < levels:
            exchange(block, piece, stage + 1).start()

    def stages(block, piece, guard):
        for stage in range(levels):
            earlier = piece - lags[stage]
            of_piece = earlier % pieces
            of_block = block + earlier // pieces
            if guard:

                @pl.when(of_block >= 0)
                def _():
                    combine(of_block, of_piece, stage)
            else:
                if of_block < blocks and of_block >= 0:
                    combine(of_block, of_piece, stage)

    def block_step(block, carry):
        for task in range(task_count):
            compute(block, task)
            for piece in range(task * halves, (task + 1) * halves):
                exchange(block, piece, 0).start()
            for piece in range(task * halves, (task + 1) * halves):
                stages(block, piece, True)
        return carry

    lax.fori_loop(0, blocks, block_step, 0)
    for tick in range(lags[-1]):
        stages(blocks + tick // pieces, tick % pieces, False)

    final = landed[levels - 1]
    row = lax.broadcasted_iota(jnp.int32, (8, 128), 0)
    lane = lax.broadcasted_iota(jnp.int32, (8, 128), 1)
    total = jnp.zeros((8, 128), jnp.float32)
    for task in range(task_count):
        here = (row == task) & (lane == task_count)
        total = jnp.where(here, loss[task : task + 1], total)
    for one in range(task_count):
        for other in range(one, task_count):
            product = 0.0
            for block in range(blocks):
                for half in range(halves):
                    base = block * pieces + half
                    product = product + final[base + one * halves] * final[base + other * halves]
            inner = jnp.sum(jnp.sum(product, axis=0, keepdims=True), axis=1, keepdims=True)
            here = ((row == one) & (lane == other)) | ((row == other) & (lane == one))
            total = jnp.where(here, inner, total)
    for level in range(shard_levels):
        pair_sum[level] = total
        copy = pltpu.make_async_remote_copy(
            src_ref=pair_sum.at[level],
            dst_ref=other_sum.at[level],
            send_sem=pair_send.at[level],
            recv_sem=pair_recv.at[level],
            device_id=(me, shard_partner[level]),
            device_id_type=MESH,
        )
        copy.start()
        copy.wait()
        total = total + other_sum[level]
    all_sums[me] = total

    def share(offset, owner):
        return pltpu.make_async_remote_copy(
            src_ref=all_sums.at[me],
            dst_ref=all_sums.at[owner],
            send_sem=share_send.at[offset - 1],
            recv_sem=share_recv.at[owner],
            device_id=((me + offset) % replicas, my_shard),
            device_id_type=MESH,
        )

    for offset in range(1, replicas):
        share(offset, me).start()
    for offset in range(1, replicas):
        share(offset, (me + offset) % replicas).wait_recv()
    for offset in range(1, replicas):
        share(offset, me).wait_send()
    total = all_sums[0]
    for device in range(1, replicas):
        total = total + all_sums[device]

    is_task = row[:, :1] < task_count
    diagonal = jnp.sum(jnp.where(row == lane, total, 0.0), axis=1, keepdims=True)
    losses = total[:, task_count : task_count + 1]

    def over_tasks(values):
        return jnp.sum(jnp.where(is_task, values, 0.0), axis=0, keepdims=True)

    def column_of(values):
        column = jnp.ones((8, 1), jnp.float32)
        for task in range(task_count):
            column = jnp.where(row[:, :1] == task, values[task], column)
        return column

    start_weights = column_of(weights)
    root_mean = jnp.sqrt(diagonal / entries + epsilon)
    scaled = start_weights * root_mean
    average = over_tasks(scaled) / task_count
    loss_ratio = losses / column_of(initial)
    relative = loss_ratio / (over_tasks(loss_ratio) / task_count)
    target = average * (relative * jnp.sqrt(relative))
    distance = (scaled - target) / average
    raised = start_weights * jnp.exp(-learn_rate * distance)
    fresh = task_count * raised / over_tasks(raised)
    fresh = jnp.where(is_task, fresh, 0.0)
    across = jnp.sum(jnp.where(row == lane, fresh, 0.0), axis=0, keepdims=True)
    renewed[...] = across[:, :task_count]
    gram = jnp.where((row < task_count) & (lane < task_count), total, 0.0)
    inner = jnp.sum(gram * across, axis=1, keepdims=True)
    mean_square = jnp.sum(inner * fresh, axis=0, keepdims=True) / entries
    gain = lax.rsqrt(mean_square + epsilon)
    for block in range(blocks):
        for half in range(halves):
            base = block * pieces + half
            combined = fresh[0:1] * final[base]
            for task in range(1, task_count):
                combined = combined + fresh[task : task + 1] * final[base + task * halves]
            start = block * columns + half * lanes
            update[:, start : start + lanes] = combined * gain


def reduce_gradients(
    features, shared, heads, labels, masks, weights, initial, replica_count, shard_count
):
    samples, width_in = features.shape
    local_hidden = shared.shape[1]
    task_count = heads.shape[0]
    levels = replica_count.bit_length() - 1
    shard_levels = shard_count.bit_length() - 1
    entries = width_in * local_hidden * shard_count
    columns = min(256, local_hidden)
    lanes = min(128, columns)
    halves = columns // lanes
    chunks = (local_hidden // columns) * task_count * halves
    slots = 3 if task_count % 3 == 0 else task_count
    pairs = max(shard_levels, 1)
    rows = width_in // replica_count
    row_block = min(ROW_BLOCK, samples)
    vmem = pl.BlockSpec(memory_space=pltpu.VMEM)
    smem = pl.BlockSpec(memory_space=pltpu.SMEM)
    anywhere = pl.BlockSpec(memory_space=pl.ANY)
    landed = [
        pltpu.VMEM((chunks,) + (2,) * (levels - 1 - stage) + (rows, lanes), jnp.float32)
        for stage in range(levels)
    ]
    return pl.pallas_call(
        functools.partial(
            reduce_kernel,
            task_count,
            levels,
            shard_levels,
            entries,
            samples * replica_count,
        ),
        out_shape=(
            jax.ShapeDtypeStruct((rows, local_hidden), jnp.float32),
            jax.ShapeDtypeStruct((1, task_count), jnp.float32),
        ),
        in_specs=[anywhere, vmem, vmem, vmem, vmem, smem, smem],
        out_specs=(vmem, vmem),
        scratch_shapes=[
            pltpu.VMEM((width_in, samples), jnp.bfloat16),
            pltpu.VMEM((2, row_block, width_in), jnp.bfloat16),
            pltpu.VMEM((samples, local_hidden), jnp.float32),
            pltpu.VMEM((samples, task_count), jnp.float32),
            pltpu.VMEM((shard_levels + 1, task_count, samples), jnp.float32),
            pltpu.VMEM((pairs, task_count, samples), jnp.float32),
            pltpu.VMEM((samples, columns), jnp.bfloat16),
            pltpu.VMEM((slots, halves) + (2,) * levels + (rows, lanes), jnp.float32),
            *landed,
            pltpu.VMEM((pairs, 8, 128), jnp.float32),
            pltpu.VMEM((pairs, 8, 128), jnp.float32),
            pltpu.VMEM((replica_count, 8, 128), jnp.float32),
            pltpu.SemaphoreType.DMA((2,)),
            pltpu.SemaphoreType.DMA((chunks, levels)),
            pltpu.SemaphoreType.DMA((chunks, levels)),
            pltpu.SemaphoreType.DMA((pairs,)),
            pltpu.SemaphoreType.DMA((pairs,)),
            pltpu.SemaphoreType.DMA((pairs,)),
            pltpu.SemaphoreType.DMA((pairs,)),
            pltpu.SemaphoreType.DMA((replica_count - 1,)),
            pltpu.SemaphoreType.DMA((replica_count,)),
        ],
        compiler_params=pltpu.CompilerParams(
            collective_id=0, has_side_effects=True, vmem_limit_bytes=67043328
        ),
        name="reduce_gradients",
    )(features, shared, heads, labels, masks, weights, initial)


def on_device(
    features, shared_weight, task_heads, labels, task_masks, task_weights, initial_losses
):
    update, renewed = reduce_gradients(
        features,
        shared_weight,
        task_heads,
        labels.T,
        task_masks.T,
        task_weights,
        initial_losses,
        lax.axis_size("dp"),
        lax.axis_size("shard"),
    )
    return (update, renewed[0])


def solution(mesh):
    return jax.shard_map(
        on_device,
        mesh=mesh,
        in_specs=(
            P("dp", None),
            P(None, "shard"),
            P(None, "shard"),
            P("dp", None),
            P("dp", None),
            P(),
            P(),
        ),
        out_specs=(P("dp", "shard"), P()),
        check_vma=False,
    )
```

```python
import functools
import jax
import jax.numpy as jnp
from jax import lax
from jax.experimental import pallas as pl
from jax.experimental.pallas import tpu as pltpu
from jax.sharding import PartitionSpec as P

epsilon = 1e-06
learn_rate = 0.5
asymmetry = 1.5
MESH = pl.DeviceIdType.MESH
LAGS = (4, 4, 8, 8, 12, 12, 16)
ROW_BLOCK = 512
FILL_ROWS = 1024


def silu_parts(preact):
    sigmoid_pre = jax.nn.sigmoid(preact)
    return (preact * sigmoid_pre, sigmoid_pre * (1.0 + preact * (1.0 - sigmoid_pre)))


def exchange_orders(count, levels):
    if levels == 4:
        table = ((0, 1, 2, 3), (1, 0, 2, 3), (2, 0, 1, 3), (0, 1, 2, 3), (1, 0, 2, 3), (2, 1, 0, 3))
        return [table[index % 6] for index in range(count)]
    return [tuple((index + level) % levels for level in range(levels)) for index in range(count)]


def stage_lags(levels):
    if levels == 4:
        return LAGS
    return tuple(4 + 4 * (step // 2) for step in range(2 * levels - 1))


def partner_of(me, bit):
    mine = (me // (1 << bit)) % 2
    return me + (1 - 2 * mine) * (1 << bit)


def reduce_kernel(
    task_count,
    levels,
    shard_levels,
    entries,
    total_samples,
    features,
    shared_hbm,
    heads,
    labels,
    masks,
    weights,
    initial,
    update,
    renewed,
    turned,
    rows_in,
    shared,
    slope,
    errors,
    logits,
    other_logits,
    even_terms,
    odd_terms,
    grads,
    *rest,
):
    landed = rest[:levels]
    pair_sum, other_sum, all_sums = rest[levels : levels + 3]
    row_sem, weight_sem, send_sem, recv_sem = rest[levels + 3 : levels + 7]
    logit_send, logit_recv, pair_send, pair_recv, share_send, share_recv = rest[levels + 7 :]
    me = lax.axis_index("dp")
    my_shard = lax.axis_index("shard")
    replicas = 1 << levels
    terms = (even_terms, odd_terms)
    hidden = odd_terms
    samples, width_in = features.shape
    local_hidden = shared.shape[1]
    columns = even_terms.shape[1]
    blocks = local_hidden // columns
    row_block = rows_in.shape[1]
    row_blocks = samples // row_block
    lanes = grads.shape[-1]
    halves = columns // lanes
    pieces = task_count * halves
    slots = grads.shape[0]
    tile = min(512, width_in)
    tiles = width_in // tile
    tile_bits = tiles.bit_length() - 1
    orders = exchange_orders(pieces, levels)
    lags = stage_lags(levels)
    dp_partner = [partner_of(me, bit) for bit in range(levels)]
    shard_partner = [partner_of(my_shard, bit) for bit in range(shard_levels)]
    my_bit = [(me // (1 << bit)) % 2 for bit in range(levels)]

    barrier = pltpu.get_barrier_semaphore()
    for offset in range(1, replicas):
        pl.semaphore_signal(
            barrier, inc=1, device_id=((me + offset) % replicas, my_shard), device_id_type=MESH
        )
    for bit in range(shard_levels):
        pl.semaphore_signal(
            barrier, inc=1, device_id=(me, shard_partner[bit]), device_id_type=MESH
        )

    def load_rows(index):
        return pltpu.make_async_copy(
            features.at[pl.ds(pl.multiple_of(index * row_block, row_block), row_block), :],
            rows_in.at[index % 2],
            row_sem.at[index % 2],
        )

    load_weight = pltpu.make_async_copy(shared_hbm, shared, weight_sem.at[0])
    load_weight.start()
    load_rows(0).start()
    load_weight.wait()

    def store_logits(index):
        partial = jnp.zeros((row_block, task_count), jnp.float32)
        for block in range(blocks):
            partial = partial + lax.dot_general(
                hidden[block * row_block : (block + 1) * row_block, :],
                heads[:, block * columns : (block + 1) * columns],
                (((1,), (1,)), ((), ())),
                preferred_element_type=jnp.float32,
            )
        rows = pl.ds(pl.multiple_of(index * row_block, row_block), row_block)
        logits[0, :, rows] = partial.T

    def front(index, carry):
        @pl.when(index + 1 < row_blocks)
        def _():
            load_rows(index + 1).start()

        load_rows(index).wait()
        inputs = rows_in[index % 2]
        rows = pl.ds(pl.multiple_of(index * row_block, row_block), row_block)
        turned[:, rows] = inputs.T
        store_logits(jnp.maximum(index - 1, 0))
        for block in range(blocks):
            part = slice(block * columns, (block + 1) * columns)
            preact = jnp.dot(inputs, shared[:, part], preferred_element_type=jnp.float32)
            activated, silu_slope = silu_parts(preact)
            slope[rows, part] = silu_slope
            hidden[block * row_block : (block + 1) * row_block, :] = activated.astype(jnp.bfloat16)
        return carry

    hidden[...] = jnp.zeros_like(hidden)
    lax.fori_loop(0, row_blocks, front, 0)
    store_logits(row_blocks - 1)
    pl.semaphore_wait(barrier, replicas - 1 + shard_levels)
    for level in range(shard_levels):
        copy = pltpu.make_async_remote_copy(
            src_ref=logits.at[level],
            dst_ref=other_logits.at[level],
            send_sem=logit_send.at[level],
            recv_sem=logit_recv.at[level],
            device_id=(me, shard_partner[level]),
            device_id_type=MESH,
        )
        copy.start()
        copy.wait()
        logits[level + 1] = logits[level] + other_logits[level]
    whole = logits[shard_levels]
    targets = labels[...].astype(jnp.float32)
    mask_float = masks[...].astype(jnp.float32)
    loss = jnp.sum(
        mask_float * (jax.nn.softplus(whole) - targets * whole), axis=1, keepdims=True
    ) / (total_samples * (1 << shard_levels))
    flat_errors = mask_float * (jax.nn.sigmoid(whole) - targets)
    errors[...] = flat_errors.T

    def fill(block, task, start, count):
        part = pl.ds(pl.multiple_of(block * columns, columns), columns)
        rows = pl.ds(pl.multiple_of(start, count), count)
        scaled = errors[rows, task : task + 1] * slope[rows, part]
        head = heads[task : task + 1, part].astype(jnp.float32)
        terms[task % 2][rows, :] = (scaled * head).astype(jnp.bfloat16)

    def fill_first(step, carry):
        fill(0, 0, step * FILL_ROWS, FILL_ROWS)
        return carry

    def compute(block, task):
        following = (task + 1) % task_count
        next_block = jnp.minimum(block + (task + 1) // task_count, blocks - 1)
        share_rows = samples // tiles

        def multiply(step, carry):
            rows = pl.ds(pl.multiple_of(step * tile, tile), tile)
            product = jnp.dot(
                turned[rows, :], terms[task % 2][...], preferred_element_type=jnp.float32
            )
            fill(next_block, following, step * share_rows, share_rows)
            high = tuple((step // (1 << bit)) % 2 for bit in range(tile_bits - 1, -1, -1))
            shape = grads.shape[2 + tile_bits :]
            for half in range(halves):
                part = product[:, half * lanes : (half + 1) * lanes]
                grads[(task % slots, half) + high] = part.reshape(shape)
            return carry

        lax.fori_loop(0, tiles, multiply, 0)

    def part_of(block, piece, stage, side):
        order = orders[piece]
        left = [bit for bit in range(levels - 1, -1, -1) if bit not in order[:stage]]
        chosen = [side if bit == order[stage] else slice(None) for bit in left]
        if stage == 0:
            return grads, ((piece // halves) % slots, piece % halves, *chosen)
        return landed[stage - 1], (block * pieces + piece, *chosen)

    def exchange(block, piece, stage):
        bit = orders[piece][stage]
        index = block * pieces + piece
        source, where = part_of(block, piece, stage, 1 - my_bit[bit])
        return pltpu.make_async_remote_copy(
            src_ref=source.at[where],
            dst_ref=landed[stage].at[index],
            send_sem=send_sem.at[index, stage],
            recv_sem=recv_sem.at[index, stage],
            device_id=(dp_partner[bit], my_shard),
            device_id_type=MESH,
        )

    def combine(block, piece, stage):
        bit = orders[piece][stage]
        index = block * pieces + piece
        exchange(block, piece, stage).wait()
        source, where = part_of(block, piece, stage, my_bit[bit])
        landed[stage][index] = landed[stage][index] + source[where]

    def advance(block, piece, step):
        if step % 2 == 0:
            combine(block, piece, step // 2)
        else:
            exchange(block, piece, (step + 1) // 2).start()

    def stages(block, piece, guard):
        for step, lag in enumerate(lags):
            earlier = piece - lag
            of_piece = earlier % pieces
            of_block = block + earlier // pieces
            if guard:

                @pl.when(of_block >= 0)
                def _():
                    advance(of_block, of_piece, step)
            else:
                if of_block < blocks and of_block >= 0:
                    advance(of_block, of_piece, step)

    def block_step(block, carry):
        for task in range(task_count):
            compute(block, task)
            for piece in range(task * halves, (task + 1) * halves):
                exchange(block, piece, 0).start()
            for piece in range(task * halves, (task + 1) * halves):
                stages(block, piece, True)
        return carry

    lax.fori_loop(0, samples // FILL_ROWS, fill_first, 0)
    lax.fori_loop(0, blocks, block_step, 0)
    for tick in range(lags[-1]):
        stages(blocks + tick // pieces, tick % pieces, False)

    final = landed[levels - 1]
    row = lax.broadcasted_iota(jnp.int32, (8, 128), 0)
    lane = lax.broadcasted_iota(jnp.int32, (8, 128), 1)
    total = jnp.zeros((8, 128), jnp.float32)
    for task in range(task_count):
        here = (row == task) & (lane == task_count)
        total = jnp.where(here, loss[task : task + 1], total)
    for one in range(task_count):
        for other in range(one, task_count):
            product = 0.0
            for block in range(blocks):
                for half in range(halves):
                    base = block * pieces + half
                    product = product + final[base + one * halves] * final[base + other * halves]
            inner = jnp.sum(jnp.sum(product, axis=0, keepdims=True), axis=1, keepdims=True)
            here = ((row == one) & (lane == other)) | ((row == other) & (lane == one))
            total = jnp.where(here, inner, total)
    for level in range(shard_levels):
        pair_sum[level] = total
        copy = pltpu.make_async_remote_copy(
            src_ref=pair_sum.at[level],
            dst_ref=other_sum.at[level],
            send_sem=pair_send.at[level],
            recv_sem=pair_recv.at[level],
            device_id=(me, shard_partner[level]),
            device_id_type=MESH,
        )
        copy.start()
        copy.wait()
        total = total + other_sum[level]
    all_sums[me] = total

    def share(offset, owner):
        return pltpu.make_async_remote_copy(
            src_ref=all_sums.at[me],
            dst_ref=all_sums.at[owner],
            send_sem=share_send.at[offset - 1],
            recv_sem=share_recv.at[owner],
            device_id=((me + offset) % replicas, my_shard),
            device_id_type=MESH,
        )

    for offset in range(1, replicas):
        share(offset, me).start()
    for offset in range(1, replicas):
        share(offset, (me + offset) % replicas).wait_recv()
    for offset in range(1, replicas):
        share(offset, me).wait_send()
    total = all_sums[0]
    for device in range(1, replicas):
        total = total + all_sums[device]

    is_task = row[:, :1] < task_count
    diagonal = jnp.sum(jnp.where(row == lane, total, 0.0), axis=1, keepdims=True)
    losses = total[:, task_count : task_count + 1]

    def over_tasks(values):
        return jnp.sum(jnp.where(is_task, values, 0.0), axis=0, keepdims=True)

    def column_of(values):
        column = jnp.ones((8, 1), jnp.float32)
        for task in range(task_count):
            column = jnp.where(row[:, :1] == task, values[task], column)
        return column

    start_weights = column_of(weights)
    root_mean = jnp.sqrt(diagonal / entries + epsilon)
    scaled = start_weights * root_mean
    average = over_tasks(scaled) / task_count
    loss_ratio = losses / column_of(initial)
    relative = loss_ratio / (over_tasks(loss_ratio) / task_count)
    target = average * (relative * jnp.sqrt(relative))
    distance = (scaled - target) / average
    raised = start_weights * jnp.exp(-learn_rate * distance)
    fresh = task_count * raised / over_tasks(raised)
    fresh = jnp.where(is_task, fresh, 0.0)
    across = jnp.sum(jnp.where(row == lane, fresh, 0.0), axis=0, keepdims=True)
    renewed[...] = across[:, :task_count]
    gram = jnp.where((row < task_count) & (lane < task_count), total, 0.0)
    inner = jnp.sum(gram * across, axis=1, keepdims=True)
    mean_square = jnp.sum(inner * fresh, axis=0, keepdims=True) / entries
    gain = lax.rsqrt(mean_square + epsilon)
    for block in range(blocks):
        for half in range(halves):
            base = block * pieces + half
            combined = fresh[0:1] * final[base]
            for task in range(1, task_count):
                combined = combined + fresh[task : task + 1] * final[base + task * halves]
            start = block * columns + half * lanes
            update[:, start : start + lanes] = combined * gain


def reduce_gradients(
    features, shared, heads, labels, masks, weights, initial, replica_count, shard_count
):
    samples, width_in = features.shape
    local_hidden = shared.shape[1]
    task_count = heads.shape[0]
    levels = replica_count.bit_length() - 1
    shard_levels = shard_count.bit_length() - 1
    entries = width_in * local_hidden * shard_count
    columns = min(256, local_hidden)
    lanes = min(128, columns)
    halves = columns // lanes
    chunks = (local_hidden // columns) * task_count * halves
    slots = 3 if task_count % 3 == 0 else task_count
    pairs = max(shard_levels, 1)
    rows = width_in // replica_count
    row_block = min(ROW_BLOCK, samples)
    vmem = pl.BlockSpec(memory_space=pltpu.VMEM)
    smem = pl.BlockSpec(memory_space=pltpu.SMEM)
    anywhere = pl.BlockSpec(memory_space=pl.ANY)
    landed = [
        pltpu.VMEM((chunks,) + (2,) * (levels - 1 - stage) + (rows, lanes), jnp.float32)
        for stage in range(levels)
    ]
    return pl.pallas_call(
        functools.partial(
            reduce_kernel,
            task_count,
            levels,
            shard_levels,
            entries,
            samples * replica_count,
        ),
        out_shape=(
            jax.ShapeDtypeStruct((rows, local_hidden), jnp.float32),
            jax.ShapeDtypeStruct((1, task_count), jnp.float32),
        ),
        in_specs=[anywhere, anywhere, vmem, vmem, vmem, smem, smem],
        out_specs=(vmem, vmem),
        scratch_shapes=[
            pltpu.VMEM((width_in, samples), jnp.bfloat16),
            pltpu.VMEM((2, row_block, width_in), jnp.bfloat16),
            pltpu.VMEM((width_in, local_hidden), jnp.bfloat16),
            pltpu.VMEM((samples, local_hidden), jnp.float32),
            pltpu.VMEM((samples, task_count), jnp.float32),
            pltpu.VMEM((shard_levels + 1, task_count, samples), jnp.float32),
            pltpu.VMEM((pairs, task_count, samples), jnp.float32),
            pltpu.VMEM((samples, columns), jnp.bfloat16),
            pltpu.VMEM((samples, columns), jnp.bfloat16),
            pltpu.VMEM((slots, halves) + (2,) * levels + (rows, lanes), jnp.float32),
            *landed,
            pltpu.VMEM((pairs, 8, 128), jnp.float32),
            pltpu.VMEM((pairs, 8, 128), jnp.float32),
            pltpu.VMEM((replica_count, 8, 128), jnp.float32),
            pltpu.SemaphoreType.DMA((2,)),
            pltpu.SemaphoreType.DMA((1,)),
            pltpu.SemaphoreType.DMA((chunks, levels)),
            pltpu.SemaphoreType.DMA((chunks, levels)),
            pltpu.SemaphoreType.DMA((pairs,)),
            pltpu.SemaphoreType.DMA((pairs,)),
            pltpu.SemaphoreType.DMA((pairs,)),
            pltpu.SemaphoreType.DMA((pairs,)),
            pltpu.SemaphoreType.DMA((replica_count - 1,)),
            pltpu.SemaphoreType.DMA((replica_count,)),
        ],
        compiler_params=pltpu.CompilerParams(
            collective_id=0, has_side_effects=True, vmem_limit_bytes=67043328
        ),
        name="reduce_gradients",
    )(features, shared, heads, labels, masks, weights, initial)


def on_device(
    features, shared_weight, task_heads, labels, task_masks, task_weights, initial_losses
):
    update, renewed = reduce_gradients(
        features,
        shared_weight,
        task_heads,
        labels.T,
        task_masks.T,
        task_weights,
        initial_losses,
        lax.axis_size("dp"),
        lax.axis_size("shard"),
    )
    return (update, renewed[0])


def solution(mesh):
    return jax.shard_map(
        on_device,
        mesh=mesh,
        in_specs=(
            P("dp", None),
            P(None, "shard"),
            P(None, "shard"),
            P("dp", None),
            P("dp", None),
            P(),
            P(),
        ),
        out_specs=(P("dp", "shard"), P()),
        check_vma=False,
    )
```

```python
import functools
import jax
import jax.numpy as jnp
from jax import lax
from jax.experimental import pallas as pl
from jax.experimental.pallas import tpu as pltpu
from jax.sharding import PartitionSpec as P

epsilon = 1e-06
learn_rate = 0.5
asymmetry = 1.5
MESH = pl.DeviceIdType.MESH
LAGS = (4, 4, 8, 8, 12, 12, 16)
ROW_BLOCK = 512
FILL_ROWS = 1024


def silu_parts(preact):
    sigmoid_pre = jax.nn.sigmoid(preact)
    return (preact * sigmoid_pre, sigmoid_pre * (1.0 + preact * (1.0 - sigmoid_pre)))


def exchange_orders(count, levels):
    if levels == 4:
        table = ((0, 1, 2, 3), (1, 0, 2, 3), (2, 0, 1, 3), (0, 1, 2, 3), (1, 0, 2, 3), (2, 1, 0, 3))
        return [table[index % 6] for index in range(count)]
    return [tuple((index + level) % levels for level in range(levels)) for index in range(count)]


def stage_lags(levels):
    if levels == 4:
        return LAGS
    return tuple(4 + 4 * (step // 2) for step in range(2 * levels - 1))


def partner_of(me, bit):
    mine = (me // (1 << bit)) % 2
    return me + (1 - 2 * mine) * (1 << bit)


def reduce_kernel(
    task_count,
    levels,
    shard_levels,
    entries,
    total_samples,
    features,
    shared_hbm,
    heads,
    labels,
    masks,
    weights,
    initial,
    update,
    renewed,
    turned,
    rows_in,
    shared,
    slope,
    errors,
    logits,
    other_logits,
    even_terms,
    odd_terms,
    grads,
    *rest,
):
    landed = rest[:levels]
    pair_sum, other_sum, all_sums = rest[levels : levels + 3]
    row_sem, weight_sem, send_sem, recv_sem = rest[levels + 3 : levels + 7]
    logit_send, logit_recv, pair_send, pair_recv, share_send, share_recv = rest[levels + 7 :]
    me = lax.axis_index("dp")
    my_shard = lax.axis_index("shard")
    replicas = 1 << levels
    terms = (even_terms, odd_terms)
    hidden = odd_terms
    samples, width_in = features.shape
    local_hidden = shared.shape[1]
    columns = even_terms.shape[1]
    blocks = local_hidden // columns
    row_block = rows_in.shape[1]
    row_blocks = samples // row_block
    lanes = grads.shape[-1]
    halves = columns // lanes
    pieces = task_count * halves
    slots = grads.shape[0]
    tile = min(512, width_in)
    tiles = width_in // tile
    tile_bits = tiles.bit_length() - 1
    orders = exchange_orders(pieces, levels)
    lags = stage_lags(levels)
    dp_partner = [partner_of(me, bit) for bit in range(levels)]
    shard_partner = [partner_of(my_shard, bit) for bit in range(shard_levels)]
    my_bit = [(me // (1 << bit)) % 2 for bit in range(levels)]

    barrier = pltpu.get_barrier_semaphore()
    for offset in range(1, replicas):
        pl.semaphore_signal(
            barrier, inc=1, device_id=((me + offset) % replicas, my_shard), device_id_type=MESH
        )
    for bit in range(shard_levels):
        pl.semaphore_signal(
            barrier, inc=1, device_id=(me, shard_partner[bit]), device_id_type=MESH
        )

    def load_rows(index):
        return pltpu.make_async_copy(
            features.at[pl.ds(pl.multiple_of(index * row_block, row_block), row_block), :],
            rows_in.at[index % 2],
            row_sem.at[index % 2],
        )

    load_weight = pltpu.make_async_copy(shared_hbm, shared, weight_sem.at[0])
    load_weight.start()
    load_rows(0).start()
    load_weight.wait()

    def store_logits(index):
        parts = [
            hidden[block * row_block : (block + 1) * row_block, :] for block in range(blocks)
        ]
        partial = lax.dot_general(
            jnp.concatenate(parts, axis=1),
            heads[...],
            (((1,), (1,)), ((), ())),
            preferred_element_type=jnp.float32,
        )
        rows = pl.ds(pl.multiple_of(index * row_block, row_block), row_block)
        logits[0, :, rows] = partial.T

    def front(index, carry):
        @pl.when(index + 1 < row_blocks)
        def _():
            load_rows(index + 1).start()

        load_rows(index).wait()
        inputs = rows_in[index % 2]
        rows = pl.ds(pl.multiple_of(index * row_block, row_block), row_block)
        turned[:, rows] = inputs.T
        store_logits(jnp.maximum(index - 1, 0))
        for block in range(blocks):
            part = slice(block * columns, (block + 1) * columns)
            preact = jnp.dot(inputs, shared[:, part], preferred_element_type=jnp.float32)
            activated, silu_slope = silu_parts(preact)
            slope[rows, part] = silu_slope
            hidden[block * row_block : (block + 1) * row_block, :] = activated.astype(jnp.bfloat16)
        return carry

    hidden[...] = jnp.zeros_like(hidden)
    lax.fori_loop(0, row_blocks, front, 0)
    store_logits(row_blocks - 1)
    pl.semaphore_wait(barrier, replicas - 1 + shard_levels)
    for level in range(shard_levels):
        copy = pltpu.make_async_remote_copy(
            src_ref=logits.at[level],
            dst_ref=other_logits.at[level],
            send_sem=logit_send.at[level],
            recv_sem=logit_recv.at[level],
            device_id=(me, shard_partner[level]),
            device_id_type=MESH,
        )
        copy.start()
        copy.wait()
        logits[level + 1] = logits[level] + other_logits[level]
    whole = logits[shard_levels]
    targets = labels[...].astype(jnp.float32)
    mask_float = masks[...].astype(jnp.float32)
    loss = jnp.sum(
        mask_float * (jax.nn.softplus(whole) - targets * whole), axis=1, keepdims=True
    ) / (total_samples * (1 << shard_levels))
    flat_errors = mask_float * (jax.nn.sigmoid(whole) - targets)
    errors[...] = flat_errors.T

    def fill(block, task, start, count):
        part = pl.ds(pl.multiple_of(block * columns, columns), columns)
        rows = pl.ds(pl.multiple_of(start, count), count)
        scaled = errors[rows, task : task + 1] * slope[rows, part]
        head = heads[task : task + 1, part].astype(jnp.float32)
        terms[task % 2][rows, :] = (scaled * head).astype(jnp.bfloat16)

    def fill_first(step, carry):
        fill(0, 0, step * FILL_ROWS, FILL_ROWS)
        return carry

    def compute(block, task):
        following = (task + 1) % task_count
        next_block = jnp.minimum(block + (task + 1) // task_count, blocks - 1)
        share_rows = samples // tiles

        def multiply(step, carry):
            rows = pl.ds(pl.multiple_of(step * tile, tile), tile)
            product = jnp.dot(
                turned[rows, :], terms[task % 2][...], preferred_element_type=jnp.float32
            )
            fill(next_block, following, step * share_rows, share_rows)
            high = tuple((step // (1 << bit)) % 2 for bit in range(tile_bits - 1, -1, -1))
            shape = grads.shape[2 + tile_bits :]
            for half in range(halves):
                part = product[:, half * lanes : (half + 1) * lanes]
                grads[(task % slots, half) + high] = part.reshape(shape)
            return carry

        lax.fori_loop(0, tiles, multiply, 0)

    def part_of(block, piece, stage, side):
        order = orders[piece]
        left = [bit for bit in range(levels - 1, -1, -1) if bit not in order[:stage]]
        chosen = [side if bit == order[stage] else slice(None) for bit in left]
        if stage == 0:
            return grads, ((piece // halves) % slots, piece % halves, *chosen)
        return landed[stage - 1], (block * pieces + piece, *chosen)

    def exchange(block, piece, stage):
        bit = orders[piece][stage]
        index = block * pieces + piece
        source, where = part_of(block, piece, stage, 1 - my_bit[bit])
        return pltpu.make_async_remote_copy(
            src_ref=source.at[where],
            dst_ref=landed[stage].at[index],
            send_sem=send_sem.at[index, stage],
            recv_sem=recv_sem.at[index, stage],
            device_id=(dp_partner[bit], my_shard),
            device_id_type=MESH,
        )

    def combine(block, piece, stage):
        bit = orders[piece][stage]
        index = block * pieces + piece
        exchange(block, piece, stage).wait()
        source, where = part_of(block, piece, stage, my_bit[bit])
        landed[stage][index] = landed[stage][index] + source[where]

    def advance(block, piece, step):
        if step % 2 == 0:
            combine(block, piece, step // 2)
        else:
            exchange(block, piece, (step + 1) // 2).start()

    def stages(block, piece, guard):
        for step, lag in enumerate(lags):
            earlier = piece - lag
            of_piece = earlier % pieces
            of_block = block + earlier // pieces
            if guard:

                @pl.when(of_block >= 0)
                def _():
                    advance(of_block, of_piece, step)
            else:
                if of_block < blocks and of_block >= 0:
                    advance(of_block, of_piece, step)

    def block_step(block, carry):
        for task in range(task_count):
            compute(block, task)
            for piece in range(task * halves, (task + 1) * halves):
                exchange(block, piece, 0).start()
            for piece in range(task * halves, (task + 1) * halves):
                stages(block, piece, True)
        return carry

    lax.fori_loop(0, samples // FILL_ROWS, fill_first, 0)
    lax.fori_loop(0, blocks, block_step, 0)
    for tick in range(lags[-1]):
        stages(blocks + tick // pieces, tick % pieces, False)

    final = landed[levels - 1]
    row = lax.broadcasted_iota(jnp.int32, (8, 128), 0)
    lane = lax.broadcasted_iota(jnp.int32, (8, 128), 1)
    total = jnp.zeros((8, 128), jnp.float32)
    for task in range(task_count):
        here = (row == task) & (lane == task_count)
        total = jnp.where(here, loss[task : task + 1], total)
    for one in range(task_count):
        for other in range(one, task_count):
            product = 0.0
            for block in range(blocks):
                for half in range(halves):
                    base = block * pieces + half
                    product = product + final[base + one * halves] * final[base + other * halves]
            inner = jnp.sum(jnp.sum(product, axis=0, keepdims=True), axis=1, keepdims=True)
            here = ((row == one) & (lane == other)) | ((row == other) & (lane == one))
            total = jnp.where(here, inner, total)
    for level in range(shard_levels):
        pair_sum[level] = total
        copy = pltpu.make_async_remote_copy(
            src_ref=pair_sum.at[level],
            dst_ref=other_sum.at[level],
            send_sem=pair_send.at[level],
            recv_sem=pair_recv.at[level],
            device_id=(me, shard_partner[level]),
            device_id_type=MESH,
        )
        copy.start()
        copy.wait()
        total = total + other_sum[level]
    all_sums[me] = total

    def share(offset, owner):
        return pltpu.make_async_remote_copy(
            src_ref=all_sums.at[me],
            dst_ref=all_sums.at[owner],
            send_sem=share_send.at[offset - 1],
            recv_sem=share_recv.at[owner],
            device_id=((me + offset) % replicas, my_shard),
            device_id_type=MESH,
        )

    for offset in range(1, replicas):
        share(offset, me).start()
    for offset in range(1, replicas):
        share(offset, (me + offset) % replicas).wait_recv()
    for offset in range(1, replicas):
        share(offset, me).wait_send()
    total = all_sums[0]
    for device in range(1, replicas):
        total = total + all_sums[device]

    is_task = row[:, :1] < task_count
    diagonal = jnp.sum(jnp.where(row == lane, total, 0.0), axis=1, keepdims=True)
    losses = total[:, task_count : task_count + 1]

    def over_tasks(values):
        return jnp.sum(jnp.where(is_task, values, 0.0), axis=0, keepdims=True)

    def column_of(values):
        column = jnp.ones((8, 1), jnp.float32)
        for task in range(task_count):
            column = jnp.where(row[:, :1] == task, values[task], column)
        return column

    start_weights = column_of(weights)
    root_mean = jnp.sqrt(diagonal / entries + epsilon)
    scaled = start_weights * root_mean
    average = over_tasks(scaled) / task_count
    loss_ratio = losses / column_of(initial)
    relative = loss_ratio / (over_tasks(loss_ratio) / task_count)
    target = average * (relative * jnp.sqrt(relative))
    distance = (scaled - target) / average
    raised = start_weights * jnp.exp(-learn_rate * distance)
    fresh = task_count * raised / over_tasks(raised)
    fresh = jnp.where(is_task, fresh, 0.0)
    across = jnp.sum(jnp.where(row == lane, fresh, 0.0), axis=0, keepdims=True)
    renewed[...] = across[:, :task_count]
    gram = jnp.where((row < task_count) & (lane < task_count), total, 0.0)
    inner = jnp.sum(gram * across, axis=1, keepdims=True)
    mean_square = jnp.sum(inner * fresh, axis=0, keepdims=True) / entries
    gain = lax.rsqrt(mean_square + epsilon)
    for block in range(blocks):
        for half in range(halves):
            base = block * pieces + half
            combined = fresh[0:1] * final[base]
            for task in range(1, task_count):
                combined = combined + fresh[task : task + 1] * final[base + task * halves]
            start = block * columns + half * lanes
            update[:, start : start + lanes] = combined * gain


def reduce_gradients(
    features, shared, heads, labels, masks, weights, initial, replica_count, shard_count
):
    samples, width_in = features.shape
    local_hidden = shared.shape[1]
    task_count = heads.shape[0]
    levels = replica_count.bit_length() - 1
    shard_levels = shard_count.bit_length() - 1
    entries = width_in * local_hidden * shard_count
    columns = min(256, local_hidden)
    lanes = min(128, columns)
    halves = columns // lanes
    chunks = (local_hidden // columns) * task_count * halves
    slots = 3 if task_count % 3 == 0 else task_count
    pairs = max(shard_levels, 1)
    rows = width_in // replica_count
    row_block = min(ROW_BLOCK, samples)
    vmem = pl.BlockSpec(memory_space=pltpu.VMEM)
    smem = pl.BlockSpec(memory_space=pltpu.SMEM)
    anywhere = pl.BlockSpec(memory_space=pl.ANY)
    landed = [
        pltpu.VMEM((chunks,) + (2,) * (levels - 1 - stage) + (rows, lanes), jnp.float32)
        for stage in range(levels)
    ]
    return pl.pallas_call(
        functools.partial(
            reduce_kernel,
            task_count,
            levels,
            shard_levels,
            entries,
            samples * replica_count,
        ),
        out_shape=(
            jax.ShapeDtypeStruct((rows, local_hidden), jnp.float32),
            jax.ShapeDtypeStruct((1, task_count), jnp.float32),
        ),
        in_specs=[anywhere, anywhere, vmem, vmem, vmem, smem, smem],
        out_specs=(vmem, vmem),
        scratch_shapes=[
            pltpu.VMEM((width_in, samples), jnp.bfloat16),
            pltpu.VMEM((2, row_block, width_in), jnp.bfloat16),
            pltpu.VMEM((width_in, local_hidden), jnp.bfloat16),
            pltpu.VMEM((samples, local_hidden), jnp.float32),
            pltpu.VMEM((samples, task_count), jnp.float32),
            pltpu.VMEM((shard_levels + 1, task_count, samples), jnp.float32),
            pltpu.VMEM((pairs, task_count, samples), jnp.float32),
            pltpu.VMEM((samples, columns), jnp.bfloat16),
            pltpu.VMEM((samples, columns), jnp.bfloat16),
            pltpu.VMEM((slots, halves) + (2,) * levels + (rows, lanes), jnp.float32),
            *landed,
            pltpu.VMEM((pairs, 8, 128), jnp.float32),
            pltpu.VMEM((pairs, 8, 128), jnp.float32),
            pltpu.VMEM((replica_count, 8, 128), jnp.float32),
            pltpu.SemaphoreType.DMA((2,)),
            pltpu.SemaphoreType.DMA((1,)),
            pltpu.SemaphoreType.DMA((chunks, levels)),
            pltpu.SemaphoreType.DMA((chunks, levels)),
            pltpu.SemaphoreType.DMA((pairs,)),
            pltpu.SemaphoreType.DMA((pairs,)),
            pltpu.SemaphoreType.DMA((pairs,)),
            pltpu.SemaphoreType.DMA((pairs,)),
            pltpu.SemaphoreType.DMA((replica_count - 1,)),
            pltpu.SemaphoreType.DMA((replica_count,)),
        ],
        compiler_params=pltpu.CompilerParams(
            collective_id=0, has_side_effects=True, vmem_limit_bytes=67043328
        ),
        name="reduce_gradients",
    )(features, shared, heads, labels, masks, weights, initial)


def on_device(
    features, shared_weight, task_heads, labels, task_masks, task_weights, initial_losses
):
    update, renewed = reduce_gradients(
        features,
        shared_weight,
        task_heads,
        labels.T,
        task_masks.T,
        task_weights,
        initial_losses,
        lax.axis_size("dp"),
        lax.axis_size("shard"),
    )
    return (update, renewed[0])


def solution(mesh):
    return jax.shard_map(
        on_device,
        mesh=mesh,
        in_specs=(
            P("dp", None),
            P(None, "shard"),
            P(None, "shard"),
            P("dp", None),
            P("dp", None),
            P(),
            P(),
        ),
        out_specs=(P("dp", "shard"), P()),
        check_vma=False,
    )
```
